256 devices in a mesh: gx: 2 (over y_lo), gy: 8 (over x, core), gz: 16 (over z, y_hi).
Axes of the slice: x: 4, y: 4 (y_hi: 2, y_lo: 2; y = y_hi * 2 + y_lo), z: 8, core: 2. Of those that a mesh axis runs over, the one named last changes fastest.
Arguments:
- head_out: bfloat16 [6144, 4096], P(('gy', 'gx'), 'gz'), may hold values from -6 to 6
- out_weight: bfloat16 [4096, 4096], P('gz', ('gx', 'gy')), may hold values from -0.09375 to 0.09375
- residual: bfloat16 [6144, 4096], P(('gy', 'gz'), 'gx'), may hold values from -84 to 84
- norm_gain: bfloat16 [4096], replicated, may hold values from 0.5 to 1.5
Outputs:
- hidden_out: bfloat16 [6144, 4096], P(('gy', 'gz'), 'gx')
- normed: bfloat16 [6144, 4096], P(('gy', 'gz'), 'gx')
The draws below stay inside these ranges and needn't reach their ends.
All inputs are finite; a program needn't handle non-finite values.
Results may differ from the reference program's by a relative error of at most 0.0098.
Values may be sent and summed in bfloat16 or wider, within the bound.
No kernel may reach another device: no remote copies, remote signals or barrier semaphores. Data moves between devices by JAX's collectives and lax.ppermute only.
A program may use at most 64 MiB of HBM per device.

```python
import math
import jax
import jax.numpy as jnp
from jax import lax

D = 4096
FEATURES = 4096
TOKENS = 6144


def draw_residual(key, part):
    key_base, key_rows, key_cols = jax.random.split(jax.random.fold_in(key, 11), 3)
    col_pos = jnp.arange(D, dtype=jnp.float32) / D
    col_ramp = jnp.exp((col_pos - 0.5) * math.log(3.0))
    col_spread = jnp.exp(jax.random.uniform(key_cols, (1, D), jnp.float32, math.log(0.5), math.log(2.0)))
    base_draw = jnp.clip(jax.random.normal(key_base, (TOKENS, D), jnp.float32), -6.0, 6.0)
    row_scale = jnp.exp(jax.random.uniform(key_rows, (TOKENS, 1), jnp.float32, math.log(0.4), math.log(4.0)))
    return (base_draw * row_scale * col_spread * col_ramp[None, :]).astype(jnp.bfloat16)


def with_spikes(result, key, source, target, parts, factor):
    owner, partner = [(jnp.arange(result.shape[axis_at]) // (result.shape[axis_at] // parts)).reshape([-1 if axis == axis_at else 1 for axis in range(result.ndim)]) for axis_at in (source, target)]
    chosen = jax.random.permutation(key, parts)[partner]
    strong = (owner == chosen) | (owner == (partner + parts // 2) % parts)
    return jnp.where(strong, factor * result, result)


def level_of(stream_key, extent, cuts, least, largest):
    gain = 1.0
    for position, parts in cuts:
        heights = jax.random.uniform(jax.random.fold_in(jax.random.fold_in(stream_key, 6), position), (parts,), jnp.float32, least / len(cuts), largest / len(cuts))
        gain = gain * jnp.repeat(jnp.exp(heights), extent[position] // parts).reshape((-1,) + (1,) * (len(extent) - 1 - position))
    return gain


def gaussian(key, extent, deviation, bound, shards=(), kind=jnp.bfloat16):
    values = deviation * jax.random.normal(key, extent, jnp.float32)
    if shards:
        values = values * level_of(key, extent, shards, -0.22, 0.18)
    return jnp.clip(values, -bound, bound).astype(kind)


def noise_with(own_key, shape, spread, most, shards, heavy, held_as=jnp.bfloat16):
    entries = spread * jax.random.normal(own_key, shape, jnp.float32)
    if shards:
        entries = entries * level_of(own_key, shape, shards, -0.22, 0.18)
    return jnp.clip(with_spikes(entries, jax.random.fold_in(own_key, 3), *heavy), -most, most).astype(held_as)


def setup_inputs(seed: int = 0) -> dict:
    key_list = jax.random.split(jax.random.key(seed), 5)
    head_out = noise_with(key_list[0], (TOKENS, FEATURES), 1.0, 6.0, ((0, 16), (1, 16)), (1, 0, 16, 2.0))
    out_weight = gaussian(key_list[1], (FEATURES, D), FEATURES ** -0.5, 0.09375, ((0, 16), (1, 16)))
    residual = draw_residual(jax.random.fold_in(key_list[4], 71), 0)
    norm_gain = jnp.clip(1.0 + 0.1 * jax.random.normal(key_list[3], (D,), jnp.float32), 0.5, 1.5).astype(jnp.bfloat16)
    return dict(head_out=head_out, out_weight=out_weight, residual=residual, norm_gain=norm_gain)


def reference(head_out, out_weight, residual, norm_gain):
    projected = jnp.dot(head_out, out_weight, preferred_element_type=jnp.float32)
    hidden = (residual.astype(jnp.float32) + projected).astype(jnp.bfloat16)
    widened = lax.optimization_barrier(hidden).astype(jnp.float32)
    inverse = lax.rsqrt(lax.optimization_barrier(jnp.mean(widened * widened, axis=1, keepdims=True)) + 1e-05)
    normed = (widened * inverse * norm_gain.astype(jnp.float32)).astype(jnp.bfloat16)
    return (hidden, normed)
```

```python
import jax
import jax.numpy as jnp
from jax import lax
from jax.experimental import pallas as pl
from jax.experimental.pallas import tpu as pltpu
from jax.sharding import Mesh
from jax.sharding import PartitionSpec as P

XS, ZS = 4, 8
GY = ("x", "c")
GZ = ("z", "yh")
FLIP = [(0, 1), (1, 0)]
CROSS = [(0, 3), (3, 0), (1, 2), (2, 1)]
BF, F32 = jnp.bfloat16, jnp.float32


def turn(size, step):
    return [(i, (i + step) % size) for i in range(size)]


def shape(*dims, dtype=BF):
    return jax.ShapeDtypeStruct(dims, dtype)


def call(body, outs, where, *args, scratch=()):
    smem = pl.BlockSpec(memory_space=pltpu.SMEM)
    vmem = pl.BlockSpec(memory_space=pltpu.VMEM)
    return pl.pallas_call(
        body,
        out_shape=outs,
        in_specs=[smem] + [vmem] * len(args),
        out_specs=jax.tree.map(lambda _: vmem, outs),
        scratch_shapes=scratch,
    )(where, *args)


def pack(where, heads, weights, mine, theirs, both):
    yh = where[3]
    part = mine.shape[0] // 4
    for block in range(4):
        to = pl.ds(block * part, part)
        own = pl.ds(pl.multiple_of((2 * block + yh) * part, part), part)
        other = pl.ds(pl.multiple_of((2 * block + 1 - yh) * part, part), part)
        mine[to, :] = heads[own, :]
        theirs[to, :] = heads[other, :]
        both[to, :] = heads[other, :]
    both[4 * part :, :] = weights[...]


def multiply(where, mine, side, cross, both, *refs):
    tiles, (zero, p1, m1, p2, m2, p3, m3, p4, m4, rows) = refs[: 4 * XS], refs[4 * XS :]
    part, depth = mine.shape[0] // 4, mine.shape[1]
    half = XS * tiles[0].shape[1]
    first = where[1]
    for source, near, far in ((0, mine, both), (1, side, cross)):
        for block in range(4):
            at = lax.rem(source * 4 + block + first, ZS)
            to = pl.ds(pl.multiple_of(at * part, part), part)
            rows[to, :depth] = near[block * part : (block + 1) * part, :]
            rows[to, depth:] = far[block * part : (block + 1) * part, :]
    left, right = rows[:, :depth], rows[:, depth:]
    width = tiles[0].shape[1]
    for t in range(2 * XS):
        out = jnp.dot(left, tiles[2 * t][...], preferred_element_type=F32)
        out += jnp.dot(right, tiles[2 * t + 1][...], preferred_element_type=F32)
        col = slice(t * width, (t + 1) * width)
        piece = [out[k * part : (k + 1) * part, :] for k in range(ZS)]
        zero[:, col] = piece[0]
        p1[:, col] = piece[1].astype(BF)
        p2[:, col] = piece[2]
        p3[:, col] = piece[3].astype(BF)
        m3[:, col] = piece[5].astype(BF)
        m2[:, col] = piece[6]
        m1[:, col] = piece[7].astype(BF)
        if t < XS:
            p4[:, col] = piece[4].astype(BF)
        else:
            m4[:, t * width - half : (t + 1) * width - half] = piece[4].astype(BF)


def relay(where, p2, m2, p3, m3, p4, m4, up, down):
    half = p4.shape[1]
    up[:, :half] = (p2[:, :half] + p3[:, :half].astype(F32) + p4[...].astype(F32)).astype(BF)
    up[:, half:] = (p2[:, half:] + p3[:, half:].astype(F32)).astype(BF)
    down[:, :half] = (m2[:, :half] + m3[:, :half].astype(F32)).astype(BF)
    down[:, half:] = (m2[:, half:] + m3[:, half:].astype(F32) + m4[...].astype(F32)).astype(BF)


def finish(where, zero, p1, m1, up, down, residual, hidden, squares):
    x, c = where[0], where[4]
    width = residual.shape[1] // (2 * XS)
    total = jnp.zeros(squares.shape, F32)
    for t in range(2 * XS):
        col = slice(t * width, (t + 1) * width)
        block = lax.rem(x + t // 2, XS) * 2 + lax.rem(c + t % 2, 2)
        to = pl.ds(pl.multiple_of(block * width, width), width)
        projected = zero[:, col]
        for ref in (p1, m1, up, down):
            projected += ref[:, col].astype(F32)
        out = (residual[:, to].astype(F32) + projected).astype(BF)
        hidden[:, to] = out
        wide = out.astype(F32)
        for lane in range(0, width, 128):
            total += wide[:, lane : lane + 128] * wide[:, lane : lane + 128]
    squares[...] = total


def normalize(where, hidden, near, far, gain, normed):
    width = hidden.shape[1]
    squares = jnp.sum(near[...] + far[...], axis=1, keepdims=True)
    inverse = lax.rsqrt(squares / (2 * width) + 1e-05)
    mine = gain[:, pl.ds(pl.multiple_of(where[2] * width, width), width)].astype(F32)
    normed[...] = (hidden[...].astype(F32) * inverse * mine).astype(BF)


def shards(head_out, out_weight, residual, norm_gain):
    x, z, yh, gx, c = (lax.axis_index(name) for name in ("x", "z", "yh", "gx", "c"))
    where = jnp.stack([x, (gx * 4 - z + ZS) % ZS, gx, yh, c]).astype(jnp.int32)
    rows, depth = head_out.shape
    cols = out_weight.shape[1]
    part = rows // 8
    width = 2 * XS * cols
    half = shape(rows // 2, depth)
    mine, theirs, both = call(
        pack, (half, half, shape(rows // 2 + depth, depth)), where, head_out, out_weight
    )
    both = lax.ppermute(both, "yh", FLIP)
    side = lax.ppermute(mine, "gx", FLIP)
    cross = lax.ppermute(theirs, ("gx", "yh"), CROSS)
    far_weight = both[rows // 2 :]
    tiles = []
    for k in range(XS):
        own = lax.ppermute(out_weight, "x", turn(XS, -k)) if k else out_weight
        far = lax.ppermute(far_weight, "x", turn(XS, -k)) if k else far_weight
        tiles += [own, far, lax.ppermute(own, "c", FLIP), lax.ppermute(far, "c", FLIP)]
    full, narrow = shape(part, width), shape(part, width // 2)
    wide = shape(part, width, dtype=F32)
    zero, p1, m1, p2, m2, p3, m3, p4, m4 = call(
        multiply,
        (wide, full, full, wide, wide, full, full, narrow, narrow),
        where, mine, side, cross, both, *tiles,
        scratch=[pltpu.VMEM((rows, 2 * depth), BF)],
    )
    p4, m4 = lax.ppermute(p4, "z", turn(ZS, 2)), lax.ppermute(m4, "z", turn(ZS, -2))
    p3, m3 = lax.ppermute(p3, "z", turn(ZS, 1)), lax.ppermute(m3, "z", turn(ZS, -1))
    p1, m1 = lax.ppermute(p1, "z", turn(ZS, 1)), lax.ppermute(m1, "z", turn(ZS, -1))
    up, down = call(relay, (full, full), where, p2, m2, p3, m3, p4, m4)
    up, down = lax.ppermute(up, "z", turn(ZS, 2)), lax.ppermute(down, "z", turn(ZS, -2))
    hidden, squares = call(
        finish, (full, shape(part, 128, dtype=F32)), where, zero, p1, m1, up, down, residual
    )
    others = lax.ppermute(squares, "gx", FLIP)
    gain = norm_gain.reshape(1, -1)
    normed = call(normalize, full, where, hidden, squares, others, gain)
    return (hidden, normed)


def solution(mesh):
    split = Mesh(mesh.devices.reshape(2, XS, 2, ZS, 2), ("gx", *GY, *GZ))
    return jax.shard_map(
        shards,
        mesh=split,
        in_specs=(P((*GY, "gx"), GZ), P(GZ, ("gx", *GY)), P((*GY, *GZ), "gx"), P()),
        out_specs=(P((*GY, *GZ), "gx"), P((*GY, *GZ), "gx")),
        check_vma=False,
    )
```

```python
import jax
import jax.numpy as jnp
from jax import lax
from jax.experimental import pallas as pl
from jax.experimental.pallas import tpu as pltpu
from jax.sharding import Mesh
from jax.sharding import PartitionSpec as P

XS, ZS = 4, 8
GY = ("x", "c")
GZ = ("z", "yh")
FLIP = [(0, 1), (1, 0)]
CROSS = [(0, 3), (3, 0), (1, 2), (2, 1)]
ACROSS = [(2 * x + c, 2 * ((x - 1 + 2 * c) % XS) + c) for x in range(XS) for c in range(2)]


def along(step):
    return [(c * ZS + z, c * ZS + (z + step - 2 * step * c) % ZS) for c in range(2) for z in range(ZS)]


BF, F32 = jnp.bfloat16, jnp.float32


def shape(*dims, dtype=BF):
    return jax.ShapeDtypeStruct(dims, dtype)


def call(body, outs, *args, scratch=(), limit=8):
    vmem = pl.BlockSpec(memory_space=pltpu.VMEM)
    return pl.pallas_call(
        body,
        out_shape=outs,
        in_specs=[vmem] * len(args),
        out_specs=jax.tree.map(lambda _: vmem, outs),
        scratch_shapes=scratch,
        compiler_params=pltpu.CompilerParams(vmem_limit_bytes=limit * 2**20),
    )(*args)


def block(ref, index, size):
    return ref.at[pl.ds(pl.multiple_of(index * size, size), size)]


def pack(heads, mine, theirs):
    yh = lax.axis_index("yh")
    part = mine.shape[0] // 4
    for at in range(4):
        mine[at * part : (at + 1) * part, :] = block(heads, 2 * at + yh, part)[...]
        theirs[at * part : (at + 1) * part, :] = block(heads, 2 * at + 1 - yh, part)[...]


def tiles_of(refs):
    own, far, own_s, far_s, own2, far2, own2_s, far2_s, own1, far1, own1_s, far1_s = refs
    x, c = lax.axis_index("x"), lax.axis_index("c")
    depth = own.shape[0]
    ahead, behind = lax.rem(x + 1 + 2 * c, XS), lax.rem(x + 3 - 2 * c, XS)
    across = lax.rem(x + 2, XS)
    return (
        (2 * x + c, own[...], far[...]),
        (2 * x + 1 - c, own_s[...], far_s[...]),
        (2 * across + c, own2[...], far2[...]),
        (2 * across + 1 - c, own2_s[...], far2_s[...]),
        (2 * ahead + c, own1[:depth, :], far1[:depth, :]),
        (2 * ahead + 1 - c, own1[depth:, :], far1[depth:, :]),
        (2 * behind + 1 - c, own1_s[:depth, :], far1_s[:depth, :]),
        (2 * behind + c, own1_s[depth:, :], far1_s[depth:, :]),
    )


def products(rows, refs, outs):
    part = outs[0].shape[0]
    for at, near, far in tiles_of(refs):
        tile = jnp.concatenate([near, far], 0)
        width = tile.shape[1]
        out = jnp.dot(rows, tile, preferred_element_type=F32)
        col = pl.ds(pl.multiple_of(at * width, width), width)
        for k, ref in enumerate(outs):
            ref[:, col] = out[k * part : (k + 1) * part, :].astype(ref.dtype)


def multiply_far(mine, side, cross, far, *refs):
    weights, (three, five, four, rest, rows) = refs[:-5], refs[-5:]
    part, depth = mine.shape[0] // 4, mine.shape[1]
    half = mine.shape[0]
    rows[:half, :depth] = mine[...]
    rows[:half, depth:] = far[...]
    rows[half:, :depth] = side[...]
    rows[half:, depth:] = cross[...]
    here = lax.axis_index("z") + (4 - lax.axis_index("gx")) * (ZS // 2)
    way = 1 - 2 * lax.axis_index("c")

    def of(step):
        return block(rows, lax.rem(here + way * step, ZS), part)[...]

    for at, step in enumerate((0, 1, 7, 2, 6)):
        rest[at * part : (at + 1) * part, :] = of(step)
    products(jnp.concatenate([of(3), of(5), of(4)], 0), weights, (three, five, four))


def multiply_near(rows, *refs):
    products(rows[...], refs[:-5], refs[-5:])


def relay(two, six, three, five, four, first, second):
    first[...] = (two[...] + three[...].astype(F32) + four[...].astype(F32)).astype(BF)
    second[...] = (six[...] + five[...].astype(F32)).astype(BF)


def finish(zero, one, seven, first, second, residual, hidden, squares):
    projected = zero[...]
    for ref in (one, seven, first, second):
        projected += ref[...].astype(F32)
    out = (residual[...].astype(F32) + projected).astype(BF)
    hidden[...] = out
    wide = out.astype(F32)
    wide *= wide
    squares[...] = sum(wide[:, lane : lane + 128] for lane in range(0, wide.shape[1], 128))


def publish(hidden, out):
    out[...] = hidden[...]


def normalize(hidden, near, far, gain, normed):
    squares = jnp.sum(near[...] + far[...], axis=1, keepdims=True)
    inverse = lax.rsqrt(squares / (2 * hidden.shape[1]) + 1e-05)
    normed[...] = (hidden[...].astype(F32) * inverse * gain[...]).astype(BF)


def shards(head_out, out_weight, residual, norm_gain):
    rows, depth = head_out.shape
    cols = out_weight.shape[1]
    part = rows // 8
    width = 2 * XS * cols
    half = shape(rows // 2, depth)
    own = out_weight
    far = lax.ppermute(own, "yh", FLIP)
    own_s = lax.ppermute(own, "c", FLIP)
    own2 = lax.ppermute(own, "x", [(x, (x + 2) % XS) for x in range(XS)])
    own1 = lax.ppermute(jnp.concatenate([own, own_s], 0), GY, ACROSS)
    mine, theirs = call(pack, (half, half), head_out)
    side = lax.ppermute(mine, "gx", FLIP)
    cross = lax.ppermute(theirs, ("gx", "yh"), CROSS)
    far_rows = lax.ppermute(theirs, "yh", FLIP)
    far_s = lax.ppermute(far, "c", FLIP)
    far2 = lax.ppermute(far, "x", [(x, (x + 2) % XS) for x in range(XS)])
    far1 = lax.ppermute(jnp.concatenate([far, far_s], 0), GY, ACROSS)
    own2_s, own1_s = lax.ppermute(own2, "c", FLIP), lax.ppermute(own1, "c", FLIP)
    far2_s, far1_s = lax.ppermute(far2, "c", FLIP), lax.ppermute(far1, "c", FLIP)
    weights = (own, far, own_s, far_s, own2, far2, own2_s, far2_s, own1, far1, own1_s, far1_s)
    full, wide = shape(part, width), shape(part, width, dtype=F32)
    three, five, four, rest = call(
        multiply_far,
        (full, full, full, shape(5 * part, 2 * depth)),
        mine, side, cross, far_rows, *weights,
        scratch=[pltpu.VMEM((rows, 2 * depth), BF)],
        limit=12,
    )
    four = lax.ppermute(four, ("c", "z"), along(2))
    three = lax.ppermute(three, ("c", "z"), along(1))
    five = lax.ppermute(five, ("c", "z"), along(-1))
    zero, one, seven, two, six = call(multiply_near, (wide, full, full, wide, wide), rest, *weights, limit=12)
    one = lax.ppermute(one, ("c", "z"), along(1))
    seven = lax.ppermute(seven, ("c", "z"), along(-1))
    first, second = call(relay, (full, full), two, six, three, five, four)
    first = lax.ppermute(first, ("c", "z"), along(2))
    second = lax.ppermute(second, ("c", "z"), along(-2))
    hidden, squares = call(
        finish, (full, shape(part, 128, dtype=F32)), zero, one, seven, first, second, residual
    )
    others = lax.ppermute(squares, "gx", FLIP)
    result = call(publish, full, hidden)
    gain = lax.dynamic_slice_in_dim(norm_gain, lax.axis_index("gx") * width, width, 0)
    normed = call(normalize, full, hidden, squares, others, gain.astype(F32).reshape(1, width))
    return (result, normed)


def solution(mesh):
    split = Mesh(mesh.devices.reshape(2, XS, 2, ZS, 2), ("gx", *GY, *GZ))

    return jax.shard_map(
        shards,
        mesh=split,
        in_specs=(P((*GY, "gx"), GZ), P(GZ, ("gx", *GY)), P((*GY, *GZ), "gx"), P()),
        out_specs=(P((*GY, *GZ), "gx"), P((*GY, *GZ), "gx")),
        check_vma=False,
    )
```

```python
import jax
import jax.numpy as jnp
from jax import lax
from jax.experimental import pallas as pl
from jax.experimental.pallas import tpu as pltpu
from jax.sharding import Mesh
from jax.sharding import PartitionSpec as P

XS, ZS = 4, 8
GY = ("x", "c")
GZ = ("z", "yh")
FLIP = [(0, 1), (1, 0)]
CROSS = [(0, 3), (3, 0), (1, 2), (2, 1)]
ACROSS = [(2 * x + c, 2 * ((x - 1 + 2 * c) % XS) + c) for x in range(XS) for c in range(2)]


def turn(step):
    return [(z, (z + step) % ZS) for z in range(ZS)]


BF, F32 = jnp.bfloat16, jnp.float32


def shape(*dims, dtype=BF):
    return jax.ShapeDtypeStruct(dims, dtype)


def call(body, outs, *args, scratch=(), limit=8):
    vmem = pl.BlockSpec(memory_space=pltpu.VMEM)
    return pl.pallas_call(
        body,
        out_shape=outs,
        in_specs=[vmem] * len(args),
        out_specs=jax.tree.map(lambda _: vmem, outs),
        scratch_shapes=scratch,
        compiler_params=pltpu.CompilerParams(vmem_limit_bytes=limit * 2**20),
    )(*args)


def block(ref, index, size):
    return ref.at[pl.ds(pl.multiple_of(index * size, size), size)]


def pack(heads, mine, theirs):
    yh = lax.axis_index("yh")
    part = mine.shape[0] // 4
    for at in range(4):
        mine[at * part : (at + 1) * part, :] = block(heads, 2 * at + yh, part)[...]
        theirs[at * part : (at + 1) * part, :] = block(heads, 2 * at + 1 - yh, part)[...]


def tiles_of(refs):
    own, far, own_s, far_s, own2, far2, own2_s, far2_s, own1, far1, own1_s, far1_s = refs
    x, c = lax.axis_index("x"), lax.axis_index("c")
    depth = own.shape[0]
    ahead, behind, across = lax.rem(x + 1 + 2 * c, XS), lax.rem(x + 3 - 2 * c, XS), lax.rem(x + 2, XS)
    return (
        (x, 0, own[...], far[...]),
        (x, 1, own_s[...], far_s[...]),
        (across, 0, own2[...], far2[...]),
        (across, 1, own2_s[...], far2_s[...]),
        (ahead, 0, own1[:depth, :], far1[:depth, :]),
        (ahead, 1, own1[depth:, :], far1[depth:, :]),
        (behind, 1, own1_s[:depth, :], far1_s[:depth, :]),
        (behind, 0, own1_s[depth:, :], far1_s[depth:, :]),
    )


def products(rows, refs, outs, halves=()):
    part = outs[0].shape[0]
    c = lax.axis_index("c")
    for at, other, near, far in tiles_of(refs):
        tile = jnp.concatenate([near, far], 0)
        width = tile.shape[1]
        out = jnp.dot(rows, tile, preferred_element_type=F32)
        core = 1 - c if other else c
        col = pl.ds(pl.multiple_of((2 * at + core) * width, width), width)
        for k, ref in enumerate(outs):
            ref[:, col] = out[k * part : (k + 1) * part, :].astype(ref.dtype)
        if halves:
            col = pl.ds(pl.multiple_of(at * width, width), width)
            halves[other][:, col] = out[len(outs) * part :, :].astype(BF)


def multiply_far(mine, side, cross, far, *refs):
    weights, (three, five, four_up, four_down, rest, rows) = refs[:-6], refs[-6:]
    part, depth = mine.shape[0] // 4, mine.shape[1]
    half = mine.shape[0]
    rows[:half, :depth] = mine[...]
    rows[:half, depth:] = far[...]
    rows[half:, :depth] = side[...]
    rows[half:, depth:] = cross[...]
    here = lax.axis_index("z") + (4 - lax.axis_index("gx")) * (ZS // 2)

    def of(step):
        return block(rows, lax.rem(here + step, ZS), part)[...]

    for at, step in enumerate((0, 1, 7, 2, 6)):
        rest[at * part : (at + 1) * part, :] = of(step)
    products(jnp.concatenate([of(3), of(5), of(4)], 0), weights, (three, five), (four_up, four_down))


def multiply_near(rows, *refs):
    products(rows[...], refs[:-5], refs[-5:])


def relay(two, six, three, five, four_up, four_down, up, down):
    width = four_up.shape[1] // XS
    c = lax.axis_index("c")
    for x in range(XS):
        col = slice(x * width, (x + 1) * width)
        mine = pl.ds(pl.multiple_of((2 * x + c) * width, width), width)
        other = pl.ds(pl.multiple_of((2 * x + 1 - c) * width, width), width)
        up[:, mine] = (two[:, mine] + three[:, mine].astype(F32) + four_up[:, col].astype(F32)).astype(BF)
        up[:, other] = (two[:, other] + three[:, other].astype(F32)).astype(BF)
        down[:, mine] = (six[:, mine] + five[:, mine].astype(F32)).astype(BF)
        down[:, other] = (six[:, other] + five[:, other].astype(F32) + four_down[:, col].astype(F32)).astype(BF)


def finish(zero, one, seven, first, second, residual, hidden, squares):
    projected = zero[...]
    for ref in (one, seven, first, second):
        projected += ref[...].astype(F32)
    out = (residual[...].astype(F32) + projected).astype(BF)
    hidden[...] = out
    wide = out.astype(F32)
    wide *= wide
    squares[...] = sum(wide[:, lane : lane + 128] for lane in range(0, wide.shape[1], 128))


def publish(hidden, out):
    out[...] = hidden[...]


def normalize(hidden, near, far, gain, normed):
    squares = jnp.sum(near[...] + far[...], axis=1, keepdims=True)
    inverse = lax.rsqrt(squares / (2 * hidden.shape[1]) + 1e-05)
    normed[...] = (hidden[...].astype(F32) * inverse * gain[...]).astype(BF)


def shards(head_out, out_weight, residual, norm_gain):
    rows, depth = head_out.shape
    cols = out_weight.shape[1]
    part = rows // 8
    width = 2 * XS * cols
    half = shape(rows // 2, depth)
    own = out_weight
    far = lax.ppermute(own, "yh", FLIP)
    own_s = lax.ppermute(own, "c", FLIP)
    own2 = lax.ppermute(own, "x", [(x, (x + 2) % XS) for x in range(XS)])
    own1 = lax.ppermute(jnp.concatenate([own, own_s], 0), GY, ACROSS)
    mine, theirs = call(pack, (half, half), head_out)
    side = lax.ppermute(mine, "gx", FLIP)
    cross = lax.ppermute(theirs, ("gx", "yh"), CROSS)
    far_rows = lax.ppermute(theirs, "yh", FLIP)
    far_s = lax.ppermute(far, "c", FLIP)
    far2 = lax.ppermute(far, "x", [(x, (x + 2) % XS) for x in range(XS)])
    far1 = lax.ppermute(jnp.concatenate([far, far_s], 0), GY, ACROSS)
    own2_s, own1_s = lax.ppermute(own2, "c", FLIP), lax.ppermute(own1, "c", FLIP)
    far2_s, far1_s = lax.ppermute(far2, "c", FLIP), lax.ppermute(far1, "c", FLIP)
    weights = (own, far, own_s, far_s, own2, far2, own2_s, far2_s, own1, far1, own1_s, far1_s)
    full, wide = shape(part, width), shape(part, width, dtype=F32)
    thin = shape(part, width // 2)
    three, five, four_up, four_down, rest = call(
        multiply_far,
        (full, full, thin, thin, shape(5 * part, 2 * depth)),
        mine, side, cross, far_rows, *weights,
        scratch=[pltpu.VMEM((rows, 2 * depth), BF)],
        limit=12,
    )
    three, five = lax.ppermute(three, "z", turn(1)), lax.ppermute(five, "z", turn(-1))
    four_up, four_down = lax.ppermute(four_up, "z", turn(2)), lax.ppermute(four_down, "z", turn(-2))
    zero, one, seven, two, six = call(multiply_near, (wide, full, full, wide, wide), rest, *weights, limit=12)
    one, seven = lax.ppermute(one, "z", turn(1)), lax.ppermute(seven, "z", turn(-1))
    first, second = call(relay, (full, full), two, six, three, five, four_up, four_down)
    first, second = lax.ppermute(first, "z", turn(2)), lax.ppermute(second, "z", turn(-2))
    hidden, squares = call(
        finish, (full, shape(part, 128, dtype=F32)), zero, one, seven, first, second, residual
    )
    others = lax.ppermute(squares, "gx", FLIP)
    result = call(publish, full, hidden)
    gain = lax.dynamic_slice_in_dim(norm_gain, lax.axis_index("gx") * width, width, 0)
    normed = call(normalize, full, hidden, squares, others, gain.astype(F32).reshape(1, width))
    return (result, normed)


def solution(mesh):
    split = Mesh(mesh.devices.reshape(2, XS, 2, ZS, 2), ("gx", *GY, *GZ))

    return jax.shard_map(
        shards,
        mesh=split,
        in_specs=(P((*GY, "gx"), GZ), P(GZ, ("gx", *GY)), P((*GY, *GZ), "gx"), P()),
        out_specs=(P((*GY, *GZ), "gx"), P((*GY, *GZ), "gx")),
        check_vma=False,
    )
```

```python
import jax
import jax.numpy as jnp
from jax import lax
from jax.experimental import pallas as pl
from jax.experimental.pallas import tpu as pltpu
from jax.sharding import Mesh
from jax.sharding import PartitionSpec as P

XS, ZS = 4, 8
GY = ("x", "c")
GZ = ("z", "yh")
FLIP = [(0, 1), (1, 0)]
CROSS = [(0, 3), (3, 0), (1, 2), (2, 1)]
ACROSS = [(2 * x + c, 2 * ((x - 1 + 2 * c) % XS) + c) for x in range(XS) for c in range(2)]


def apart(step):
    return [(c * ZS + z, c * ZS + (z + step - 2 * step * c) % ZS) for c in range(2) for z in range(ZS)]


BF, F32 = jnp.bfloat16, jnp.float32


def shape(*dims, dtype=BF):
    return jax.ShapeDtypeStruct(dims, dtype)


def call(body, outs, *args, scratch=(), limit=8):
    vmem = pl.BlockSpec(memory_space=pltpu.VMEM)
    return pl.pallas_call(
        body,
        out_shape=outs,
        in_specs=[vmem] * len(args),
        out_specs=jax.tree.map(lambda _: vmem, outs),
        scratch_shapes=scratch,
        compiler_params=pltpu.CompilerParams(vmem_limit_bytes=limit * 2**20),
    )(*args)


def block(ref, index, size):
    return ref.at[pl.ds(pl.multiple_of(index * size, size), size)]


def pack(heads, mine, theirs):
    yh = lax.axis_index("yh")
    part = mine.shape[0] // 4
    for at in range(4):
        mine[at * part : (at + 1) * part, :] = block(heads, 2 * at + yh, part)[...]
        theirs[at * part : (at + 1) * part, :] = block(heads, 2 * at + 1 - yh, part)[...]


def tiles_of(refs):
    own, far, own_s, far_s, own2, far2, own2_s, far2_s, own1, far1, own1_s, far1_s = refs
    x, c = lax.axis_index("x"), lax.axis_index("c")
    depth = own.shape[0]
    ahead, behind, across = lax.rem(x + 1 + 2 * c, XS), lax.rem(x + 3 - 2 * c, XS), lax.rem(x + 2, XS)
    return (
        (x, 0, own[...], far[...]),
        (x, 1, own_s[...], far_s[...]),
        (across, 0, own2[...], far2[...]),
        (across, 1, own2_s[...], far2_s[...]),
        (ahead, 0, own1[:depth, :], far1[:depth, :]),
        (ahead, 1, own1[depth:, :], far1[depth:, :]),
        (behind, 1, own1_s[:depth, :], far1_s[:depth, :]),
        (behind, 0, own1_s[depth:, :], far1_s[depth:, :]),
    )


def products(rows, refs, outs, halves=()):
    part = outs[0].shape[0]
    c = lax.axis_index("c")
    for at, other, near, far in tiles_of(refs):
        tile = jnp.concatenate([near, far], 0)
        width = tile.shape[1]
        out = jnp.dot(rows, tile, preferred_element_type=F32)
        core = 1 - c if other else c
        col = pl.ds(pl.multiple_of((2 * at + core) * width, width), width)
        for k, ref in enumerate(outs):
            ref[:, col] = out[k * part : (k + 1) * part, :].astype(ref.dtype)
        if halves:
            col = pl.ds(pl.multiple_of(at * width, width), width)
            halves[other][:, col] = out[len(outs) * part :, :].astype(BF)


def multiply_far(mine, side, cross, far, *refs):
    weights, (three, five, four_up, four_down, rest, rows) = refs[:-6], refs[-6:]
    part, depth = mine.shape[0] // 4, mine.shape[1]
    half = mine.shape[0]
    rows[:half, :depth] = mine[...]
    rows[:half, depth:] = far[...]
    rows[half:, :depth] = side[...]
    rows[half:, depth:] = cross[...]
    here = lax.axis_index("z") + (4 - lax.axis_index("gx")) * (ZS // 2)

    def of(step):
        return block(rows, lax.rem(here + step, ZS), part)[...]

    way = 1 - 2 * lax.axis_index("c")
    for at, step in enumerate((0, 4 - 3 * way, 4 + 3 * way, 2, 6)):
        rest[at * part : (at + 1) * part, :] = of(step)
    products(jnp.concatenate([of(4 - way), of(4 + way), of(4)], 0), weights, (three, five), (four_up, four_down))


def multiply_near(rows, *refs):
    products(rows[...], refs[:-5], refs[-5:])


def relay(two, six, three, five, four_up, four_down, up, down):
    width = four_up.shape[1] // XS
    c = lax.axis_index("c")
    below = jnp.full((two.shape[0], width), c, jnp.int32) == 0
    for x in range(XS):
        col = slice(x * width, (x + 1) * width)
        mine = pl.ds(pl.multiple_of((2 * x + c) * width, width), width)
        other = pl.ds(pl.multiple_of((2 * x + 1 - c) * width, width), width)
        for at, extra, first in ((mine, four_up, below), (other, four_down, ~below)):
            a, b = three[:, at].astype(F32), five[:, at].astype(F32)
            extra = extra[:, col].astype(F32)
            total_up = two[:, at] + jnp.where(below, a, b) + jnp.where(first, extra, 0.0)
            total_down = six[:, at] + jnp.where(below, b, a) + jnp.where(first, 0.0, extra)
            up[:, at] = jnp.where(below, total_up, total_down).astype(BF)
            down[:, at] = jnp.where(below, total_down, total_up).astype(BF)


def finish(zero, one, seven, first, second, residual, hidden, squares):
    projected = zero[...]
    for ref in (one, seven, first, second):
        projected += ref[...].astype(F32)
    out = (residual[...].astype(F32) + projected).astype(BF)
    hidden[...] = out
    wide = out.astype(F32)
    wide *= wide
    squares[...] = sum(wide[:, lane : lane + 128] for lane in range(0, wide.shape[1], 128))


def publish(hidden, out):
    out[...] = hidden[...]


def normalize(hidden, near, far, gain, normed):
    squares = jnp.sum(near[...] + far[...], axis=1, keepdims=True)
    inverse = lax.rsqrt(squares / (2 * hidden.shape[1]) + 1e-05)
    normed[...] = (hidden[...].astype(F32) * inverse * gain[...]).astype(BF)


def shards(head_out, out_weight, residual, norm_gain):
    rows, depth = head_out.shape
    cols = out_weight.shape[1]
    part = rows // 8
    width = 2 * XS * cols
    half = shape(rows // 2, depth)
    own = out_weight
    far = lax.ppermute(own, "yh", FLIP)
    own_s = lax.ppermute(own, "c", FLIP)
    own2 = lax.ppermute(own, "x", [(x, (x + 2) % XS) for x in range(XS)])
    own1 = lax.ppermute(jnp.concatenate([own, own_s], 0), GY, ACROSS)
    mine, theirs = call(pack, (half, half), head_out)
    side = lax.ppermute(mine, "gx", FLIP)
    cross = lax.ppermute(theirs, ("gx", "yh"), CROSS)
    far_rows = lax.ppermute(theirs, "yh", FLIP)
    far_s = lax.ppermute(far, "c", FLIP)
    far2 = lax.ppermute(far, "x", [(x, (x + 2) % XS) for x in range(XS)])
    far1 = lax.ppermute(jnp.concatenate([far, far_s], 0), GY, ACROSS)
    own2_s, own1_s = lax.ppermute(own2, "c", FLIP), lax.ppermute(own1, "c", FLIP)
    far2_s, far1_s = lax.ppermute(far2, "c", FLIP), lax.ppermute(far1, "c", FLIP)
    weights = (own, far, own_s, far_s, own2, far2, own2_s, far2_s, own1, far1, own1_s, far1_s)
    full, wide = shape(part, width), shape(part, width, dtype=F32)
    thin = shape(part, width // 2)
    three, five, four_up, four_down, rest = call(
        multiply_far,
        (full, full, thin, thin, shape(5 * part, 2 * depth)),
        mine, side, cross, far_rows, *weights,
        scratch=[pltpu.VMEM((rows, 2 * depth), BF)],
        limit=12,
    )
    three, five = lax.ppermute(three, ("c", "z"), apart(1)), lax.ppermute(five, ("c", "z"), apart(-1))
    four_up, four_down = lax.ppermute(four_up, ("c", "z"), apart(2)), lax.ppermute(four_down, ("c", "z"), apart(-2))
    zero, one, seven, two, six = call(multiply_near, (wide, full, full, wide, wide), rest, *weights, limit=12)
    one, seven = lax.ppermute(one, ("c", "z"), apart(1)), lax.ppermute(seven, ("c", "z"), apart(-1))
    first, second = call(relay, (full, full), two, six, three, five, four_up, four_down)
    first, second = lax.ppermute(first, ("c", "z"), apart(2)), lax.ppermute(second, ("c", "z"), apart(-2))
    hidden, squares = call(
        finish, (full, shape(part, 128, dtype=F32)), zero, one, seven, first, second, residual
    )
    others = lax.ppermute(squares, "gx", FLIP)
    result = call(publish, full, hidden)
    gain = lax.dynamic_slice_in_dim(norm_gain, lax.axis_index("gx") * width, width, 0)
    normed = call(normalize, full, hidden, squares, others, gain.astype(F32).reshape(1, width))
    return (result, normed)


def solution(mesh):
    split = Mesh(mesh.devices.reshape(2, XS, 2, ZS, 2), ("gx", *GY, *GZ))

    return jax.shard_map(
        shards,
        mesh=split,
        in_specs=(P((*GY, "gx"), GZ), P(GZ, ("gx", *GY)), P((*GY, *GZ), "gx"), P()),
        out_specs=(P((*GY, *GZ), "gx"), P((*GY, *GZ), "gx")),
        check_vma=False,
    )
```

```python
import jax
import jax.numpy as jnp
from jax import lax
from jax.experimental import pallas as pl
from jax.experimental.pallas import tpu as pltpu
from jax.sharding import Mesh
from jax.sharding import PartitionSpec as P

XS, ZS = 4, 8
GY = ("x", "c")
GZ = ("z", "yh")
FLIP = [(0, 1), (1, 0)]
CROSS = [(0, 3), (3, 0), (1, 2), (2, 1)]
ACROSS = [(2 * x + c, 2 * ((x - 1 + 2 * c) % XS) + c) for x in range(XS) for c in range(2)]


def apart(step):
    return [(c * ZS + z, c * ZS + (z + step - 2 * step * c) % ZS) for c in range(2) for z in range(ZS)]


BF, F32 = jnp.bfloat16, jnp.float32


def shape(*dims, dtype=BF):
    return jax.ShapeDtypeStruct(dims, dtype)


def call(body, outs, *args, scratch=(), limit=8):
    vmem = pl.BlockSpec(memory_space=pltpu.VMEM)
    return pl.pallas_call(
        body,
        out_shape=outs,
        in_specs=[vmem] * len(args),
        out_specs=jax.tree.map(lambda _: vmem, outs),
        scratch_shapes=scratch,
        compiler_params=pltpu.CompilerParams(vmem_limit_bytes=limit * 2**20),
    )(*args)


def block(ref, index, size):
    return ref.at[pl.ds(pl.multiple_of(index * size, size), size)]


def pair(own, other, both):
    depth = own.shape[0]
    both[:depth, :] = own[...]
    both[depth:, :] = other[...]


def pack(heads, mine, theirs):
    yh = lax.axis_index("yh")
    part = mine.shape[0] // 4
    for at in range(4):
        mine[at * part : (at + 1) * part, :] = block(heads, 2 * at + yh, part)[...]
        theirs[at * part : (at + 1) * part, :] = block(heads, 2 * at + 1 - yh, part)[...]


def tiles_of(refs):
    own, far, own_s, far_s, own2, far2, own2_s, far2_s, own1, far1, own1_s, far1_s = refs
    x, c = lax.axis_index("x"), lax.axis_index("c")
    depth = own.shape[0]
    ahead, behind, across = lax.rem(x + 1 + 2 * c, XS), lax.rem(x + 3 - 2 * c, XS), lax.rem(x + 2, XS)
    return (
        (x, 0, own[...], far[...]),
        (x, 1, own_s[...], far_s[...]),
        (across, 0, own2[...], far2[...]),
        (across, 1, own2_s[...], far2_s[...]),
        (ahead, 0, own1[:depth, :], far1[:depth, :]),
        (ahead, 1, own1[depth:, :], far1[depth:, :]),
        (behind, 1, own1_s[:depth, :], far1_s[:depth, :]),
        (behind, 0, own1_s[depth:, :], far1_s[depth:, :]),
    )


def products(rows, refs, outs, halves=()):
    part = outs[0].shape[0]
    c = lax.axis_index("c")
    for at, other, near, far in tiles_of(refs):
        tile = jnp.concatenate([near, far], 0)
        width = tile.shape[1]
        out = jnp.dot(rows, tile, preferred_element_type=F32)
        core = 1 - c if other else c
        col = pl.ds(pl.multiple_of((2 * at + core) * width, width), width)
        for k, ref in enumerate(outs):
            ref[:, col] = out[k * part : (k + 1) * part, :].astype(ref.dtype)
        if halves:
            col = pl.ds(pl.multiple_of(at * width, width), width)
            halves[other][:, col] = out[len(outs) * part :, :].astype(BF)


def multiply_far(mine, side, cross, far, *refs):
    weights, (three, five, four_up, four_down, rest, rows) = refs[:-6], refs[-6:]
    part, depth = mine.shape[0] // 4, mine.shape[1]
    half = mine.shape[0]
    rows[:half, :depth] = mine[...]
    rows[:half, depth:] = far[...]
    rows[half:, :depth] = side[...]
    rows[half:, depth:] = cross[...]
    here = lax.axis_index("z") + (4 - lax.axis_index("gx")) * (ZS // 2)

    def of(step):
        return block(rows, lax.rem(here + step, ZS), part)[...]

    way = 1 - 2 * lax.axis_index("c")
    for at, step in enumerate((0, 4 - 3 * way, 4 + 3 * way, 2, 6)):
        rest[at * part : (at + 1) * part, :] = of(step)
    products(jnp.concatenate([of(4 - way), of(4 + way), of(4)], 0), weights, (three, five), (four_up, four_down))


def multiply_near(rows, *refs):
    products(rows[...], refs[:-5], refs[-5:])


def relay(two, six, three, five, four_up, four_down, up, down):
    width = four_up.shape[1] // XS
    c = lax.axis_index("c")
    below = jnp.full((two.shape[0], width), c, jnp.int32) == 0
    for x in range(XS):
        col = slice(x * width, (x + 1) * width)
        mine = pl.ds(pl.multiple_of((2 * x + c) * width, width), width)
        other = pl.ds(pl.multiple_of((2 * x + 1 - c) * width, width), width)
        for at, extra, first in ((mine, four_up, below), (other, four_down, ~below)):
            a, b = three[:, at].astype(F32), five[:, at].astype(F32)
            extra = extra[:, col].astype(F32)
            total_up = two[:, at] + jnp.where(below, a, b) + jnp.where(first, extra, 0.0)
            total_down = six[:, at] + jnp.where(below, b, a) + jnp.where(first, 0.0, extra)
            up[:, at] = jnp.where(below, total_up, total_down).astype(BF)
            down[:, at] = jnp.where(below, total_down, total_up).astype(BF)


def finish(zero, one, seven, first, second, residual, hidden, squares):
    projected = zero[...]
    for ref in (one, seven, first, second):
        projected += ref[...].astype(F32)
    out = (residual[...].astype(F32) + projected).astype(BF)
    hidden[...] = out
    wide = out.astype(F32)
    wide *= wide
    squares[...] = sum(wide[:, lane : lane + 128] for lane in range(0, wide.shape[1], 128))


def publish(hidden, out):
    out[...] = hidden[...]


def normalize(hidden, near, far, gain, normed):
    squares = jnp.sum(near[...] + far[...], axis=1, keepdims=True)
    inverse = lax.rsqrt(squares / (2 * hidden.shape[1]) + 1e-05)
    normed[...] = (hidden[...].astype(F32) * inverse * gain[...]).astype(BF)


def shards(head_out, out_weight, residual, norm_gain):
    rows, depth = head_out.shape
    cols = out_weight.shape[1]
    part = rows // 8
    width = 2 * XS * cols
    half = shape(rows // 2, depth)
    own = out_weight
    far = lax.ppermute(own, "yh", FLIP)
    own_s = lax.ppermute(own, "c", FLIP)
    own2 = lax.ppermute(own, "x", [(x, (x + 2) % XS) for x in range(XS)])
    own1 = lax.ppermute(call(pair, shape(2 * depth, cols), own, own_s), GY, ACROSS)
    mine, theirs = call(pack, (half, half), head_out)
    side = lax.ppermute(mine, "gx", FLIP)
    cross = lax.ppermute(theirs, ("gx", "yh"), CROSS)
    far_rows = lax.ppermute(theirs, "yh", FLIP)
    far_s = lax.ppermute(far, "c", FLIP)
    far2 = lax.ppermute(far, "x", [(x, (x + 2) % XS) for x in range(XS)])
    far1 = lax.ppermute(call(pair, shape(2 * depth, cols), far, far_s), GY, ACROSS)
    own2_s, own1_s = lax.ppermute(own2, "c", FLIP), lax.ppermute(own1, "c", FLIP)
    far2_s, far1_s = lax.ppermute(far2, "c", FLIP), lax.ppermute(far1, "c", FLIP)
    weights = (own, far, own_s, far_s, own2, far2, own2_s, far2_s, own1, far1, own1_s, far1_s)
    full, wide = shape(part, width), shape(part, width, dtype=F32)
    thin = shape(part, width // 2)
    three, five, four_up, four_down, rest = call(
        multiply_far,
        (full, full, thin, thin, shape(5 * part, 2 * depth)),
        mine, side, cross, far_rows, *weights,
        scratch=[pltpu.VMEM((rows, 2 * depth), BF)],
        limit=12,
    )
    three, five = lax.ppermute(three, ("c", "z"), apart(1)), lax.ppermute(five, ("c", "z"), apart(-1))
    four_up, four_down = lax.ppermute(four_up, ("c", "z"), apart(2)), lax.ppermute(four_down, ("c", "z"), apart(-2))
    zero, one, seven, two, six = call(multiply_near, (wide, full, full, wide, wide), rest, *weights, limit=12)
    one, seven = lax.ppermute(one, ("c", "z"), apart(1)), lax.ppermute(seven, ("c", "z"), apart(-1))
    first, second = call(relay, (full, full), two, six, three, five, four_up, four_down)
    first, second = lax.ppermute(first, ("c", "z"), apart(2)), lax.ppermute(second, ("c", "z"), apart(-2))
    hidden, squares = call(
        finish, (full, shape(part, 128, dtype=F32)), zero, one, seven, first, second, residual
    )
    others = lax.ppermute(squares, "gx", FLIP)
    result = call(publish, full, hidden)
    gain = lax.dynamic_slice_in_dim(norm_gain, lax.axis_index("gx") * width, width, 0)
    normed = call(normalize, full, hidden, squares, others, gain.astype(F32).reshape(1, width))
    return (result, normed)


def solution(mesh):
    split = Mesh(mesh.devices.reshape(2, XS, 2, ZS, 2), ("gx", *GY, *GZ))

    return jax.shard_map(
        shards,
        mesh=split,
        in_specs=(P((*GY, "gx"), GZ), P(GZ, ("gx", *GY)), P((*GY, *GZ), "gx"), P()),
        out_specs=(P((*GY, *GZ), "gx"), P((*GY, *GZ), "gx")),
        check_vma=False,
    )
```
